32 devices in a mesh: crop: 1, row: 32 (over z, y, x, core).
Axes of the slice: x: 2, y: 2, z: 4, core: 2. Of those that a mesh axis runs over, the one named last changes fastest.
Arguments:
- queries: bfloat16 [128, 128, 128], P(('crop', 'row')), may hold values from -4 to 4
- keys: bfloat16 [128, 128, 128], P(('crop', 'row')), may hold values from -4 to 4
- values: bfloat16 [128, 128, 128], P(('crop', 'row')), may hold values from -6 to 6
- grads_out: bfloat16 [128, 128, 128], P(('crop', 'row')), may hold values from -96 to 96
- log_norm: float32 [128, 4, 128], P(('crop', 'row')), may hold values from -90 to 102, as said below
- bias: bfloat16 [128, 4, 128], P(('crop', 'row')), may hold values from -4 to 4
Outputs:
- query_grad: bfloat16 [128, 128, 128], P(('crop', 'row'))
- key_grad: bfloat16 [128, 128, 128], P(('crop', 'row'))
- value_grad: bfloat16 [128, 128, 128], P(('crop', 'row'))
- bias_grad: float32 [128, 4, 128], P(('crop', 'row'))
The draws below stay inside these ranges and needn't reach their ends.
Inputs may be any that keep to these rules, and one draw needn't show every extreme that they name: log_norm[i, h, j] is the logarithm of the sum over k of exp(scores[i, h, j, k]), scores computed from the given queries, keys and bias.
All inputs are finite; a program needn't handle non-finite values.
Results may differ from the reference program's by a relative error of at most 0.0051.
Values may be sent and summed in bfloat16 or wider, within the bound.
A program may use at most 64 MiB of HBM per device.

```python
import jax
import jax.numpy as jnp
from jax import lax

HEADS = 4
HEAD_DIM = 32
TOKENS = 128
CHANNELS = 128


def shared_fields(key):
    channels = HEADS * HEAD_DIM
    shape = (TOKENS, TOKENS, channels)
    query_field = jnp.clip(jax.random.normal(jax.random.fold_in(key, 101), shape, jnp.float32), -4.0, 4.0)
    key_field = jnp.clip(jax.random.normal(jax.random.fold_in(key, 103), shape, jnp.float32), -4.0, 4.0)
    bias_field = jnp.clip(jax.random.normal(jax.random.fold_in(key, 104), (TOKENS, HEADS, TOKENS), jnp.float32), -4.0, 4.0)
    return (query_field, key_field, bias_field)


def draw_queries(key, part):
    return shared_fields(key)[0].astype(jnp.bfloat16)


def draw_keys(key, part):
    return shared_fields(key)[1].astype(jnp.bfloat16)


def draw_bias(key, part):
    return shared_fields(key)[2].astype(jnp.bfloat16)


def draw_log_norm(key, part):
    query_field, key_field, bias_field = shared_fields(key)
    query_field = query_field.astype(jnp.bfloat16).astype(jnp.float32)
    key_field = key_field.astype(jnp.bfloat16).astype(jnp.float32)
    bias_heads = jnp.transpose(bias_field.astype(jnp.bfloat16).astype(jnp.float32), (1, 0, 2))
    score_scale = HEAD_DIM ** (-0.5)

    def one_row(inputs):
        query_row, key_row = inputs
        query_heads = query_row.reshape(TOKENS, HEADS, HEAD_DIM)
        key_heads = key_row.reshape(TOKENS, HEADS, HEAD_DIM)
        scores = jnp.einsum('jhd,khd->hjk', query_heads, key_heads) * score_scale + bias_heads
        return jax.scipy.special.logsumexp(scores, axis=-1)
    return lax.map(one_row, (query_field, key_field))


def raised(drawn, key, source, target, parts, factor):
    def block_of(dim):
        return (jnp.arange(drawn.shape[dim]) // (drawn.shape[dim] // parts)).reshape((-1,) + (1,) * (drawn.ndim - 1 - dim))

    near = jax.random.permutation(key, parts)[block_of(target)]
    far = (block_of(target) + parts // 2) % parts
    return jnp.where((block_of(source) == near) | (block_of(source) == far), factor * drawn, drawn)


def shard_levels(stream_key, shape, pieces, low, top_value):
    level, own = 1.0, jax.random.fold_in(stream_key, 6)
    for axis_at, blocks in pieces:
        draws = jnp.exp(jax.random.uniform(jax.random.fold_in(own, axis_at), (blocks,), jnp.float32, low / len(pieces), top_value / len(pieces)))
        level = level * jnp.repeat(draws, shape[axis_at] // blocks).reshape([-1 if axis == axis_at else 1 for axis in range(len(shape))])
    return level


def gaussian(key, dims, deviation, limit, cuts=(), held_as=jnp.bfloat16):
    array = deviation * jax.random.normal(key, dims, jnp.float32)
    if cuts:
        array = array * shard_levels(key, dims, cuts, -0.22, 0.18)
    return jnp.clip(array, -limit, limit).astype(held_as)


def noise_with(key, dims, deviation, limit, shards, heavy, dtype=jnp.bfloat16):
    result = deviation * jax.random.normal(key, dims, jnp.float32)
    if shards:
        result = result * shard_levels(key, dims, shards, -0.22, 0.18)
    return jnp.clip(raised(result, jax.random.fold_in(key, 3), *heavy), -limit, limit).astype(dtype)


def setup_inputs(seed: int = 0, part: int = 0) -> dict:
    seeds = jax.random.split(jax.random.key(seed), 7)
    own_keys = jax.random.split(jax.random.fold_in(seeds[6], part), 7)
    queries = draw_queries(jax.random.fold_in(jax.random.fold_in(seeds[6], part), 71), part)
    keys = draw_keys(jax.random.fold_in(jax.random.fold_in(seeds[6], part), 71), part)
    values = gaussian(own_keys[2], (TOKENS, TOKENS, CHANNELS), 1.0, 6.0, ((0, 32),))
    grads_out = noise_with(own_keys[3], (TOKENS, TOKENS, CHANNELS), 16.0, 96.0, ((0, 32),), (0, 1, 32, 2.75))
    log_norm = draw_log_norm(jax.random.fold_in(jax.random.fold_in(seeds[6], part), 71), part)
    bias = draw_bias(jax.random.fold_in(jax.random.fold_in(seeds[6], part), 71), part)
    return dict(queries=queries, keys=keys, values=values, grads_out=grads_out, log_norm=log_norm, bias=bias)


def reference(queries, keys, values, grads_out, log_norm, bias):
    length = queries.shape[1]
    head_count = bias.shape[1]
    pair_width = queries.shape[2]
    head_width = pair_width // head_count
    score_scale = head_width ** -0.5
    bias_heads = jnp.transpose(bias, (1, 0, 2)).astype(jnp.float32)

    def one_row(running, inputs):
        query_row, key_row, value_row, grad_row, norm_row = inputs
        query_heads = query_row.astype(jnp.float32).reshape(length, head_count, head_width)
        key_heads = key_row.astype(jnp.float32).reshape(length, head_count, head_width)
        value_heads = value_row.astype(jnp.float32).reshape(length, head_count, head_width)
        grad_heads = grad_row.astype(jnp.float32).reshape(length, head_count, head_width)
        scores = jnp.einsum("jhd,khd->hjk", query_heads, key_heads) * score_scale + bias_heads
        weights = jnp.exp(scores - norm_row[:, :, None])
        weight_grads = jnp.einsum("jhd,khd->hjk", grad_heads, value_heads)
        centre = jnp.sum(weights * weight_grads, axis=-1, keepdims=True)
        score_grads = weights * (weight_grads - centre)
        weights_low = lax.optimization_barrier(weights.astype(jnp.bfloat16)).astype(jnp.float32)
        grads_low = lax.optimization_barrier(score_grads.astype(jnp.bfloat16)).astype(jnp.float32)
        query_part = jnp.einsum("hjk,khd->jhd", grads_low, key_heads) * score_scale
        key_part = jnp.einsum("hjk,jhd->khd", grads_low, query_heads) * score_scale
        value_part = jnp.einsum("hjk,jhd->khd", weights_low, grad_heads)
        outputs = (query_part.reshape(length, pair_width).astype(jnp.bfloat16),
                   key_part.reshape(length, pair_width).astype(jnp.bfloat16),
                   value_part.reshape(length, pair_width).astype(jnp.bfloat16))
        return running + score_grads, outputs

    start_total = jnp.zeros((head_count, length, length), jnp.float32)
    total, grads = lax.scan(one_row, start_total, (queries, keys, values, grads_out, log_norm))
    return grads[0], grads[1], grads[2], jnp.transpose(total, (1, 0, 2))
```

```python
import functools
import math

import jax
import jax.numpy as jnp
from jax import lax
from jax.experimental import pallas as pl
from jax.experimental.pallas import tpu as pltpu
from jax.sharding import PartitionSpec as P

F32 = jnp.float32
BF16 = jnp.bfloat16


def peers(me, count, body):
    def step(d, carry):
        body(d, lax.rem(me + d, count))
        return carry

    lax.fori_loop(1, count, step, 0)


def kernel(
    count, heads,
    q_hbm, k_hbm, v_hbm, g_hbm, norm_hbm, bias_hbm,
    qg_ref, kg_ref, vg_ref, bg_ref,
    q, k, v, g, norm, gath, qm, gm, kt, e1, dp, eb, p_low, s_low, wide, terms, landed,
    in_sem, gath_send, gath_recv, term_send, term_recv,
):
    me = lax.axis_index("row")
    rows, length, channels = q.shape
    width = channels // heads
    block = bias_hbm.shape[0]
    lanes = wide.shape[2]
    scale = width ** (-0.5)
    own = pl.ds(pl.multiple_of(me * block, block), block)

    barrier = pltpu.get_barrier_semaphore()
    peers(me, count, lambda d, t: pl.semaphore_signal(barrier, inc=1, device_id={"row": t}))

    pairs = ((bias_hbm, gath.at[own]), (q_hbm, q), (k_hbm, k), (v_hbm, v), (g_hbm, g), (norm_hbm, norm))
    copies = [pltpu.make_async_copy(a, b, in_sem.at[i]) for i, (a, b) in enumerate(pairs)]
    for copy in copies:
        copy.start()
    copies[0].wait()
    pl.semaphore_wait(barrier, count - 1)

    def gather_copy(t):
        return pltpu.make_async_remote_copy(
            src_ref=gath.at[own], dst_ref=gath.at[own], send_sem=gath_send, recv_sem=gath_recv,
            device_id={"row": t},
        )

    peers(me, count, lambda d, t: gather_copy(t).start())

    for copy in copies[1:]:
        copy.wait()
    channel = lax.broadcasted_iota(jnp.int32, (1, channels), 1)
    masks = [
        jnp.where((channel >= h * width) & (channel < (h + 1) * width), 1.0, 0.0).astype(BF16)
        for h in range(heads)
    ]
    nt = (((1,), (1,)), ((), ()))
    for i in range(rows):
        for h in range(heads):
            span = pl.ds(h * length, length)
            qm[i, span, :] = q[i] * masks[h]
            gm[i, span, :] = g[i] * masks[h]
        kt[i] = k[i].astype(F32).T.astype(BF16)
        score = lax.dot_general(k[i], qm[i], nt, preferred_element_type=F32)
        grad = lax.dot_general(v[i], gm[i], nt, preferred_element_type=F32)
        dp[i] = grad
        for h in range(heads):
            line = norm[pl.ds(i * heads + h, 1), :]
            tile = score[:, h * length:(h + 1) * length]
            e1[i, :, pl.ds(h * length, length)] = jnp.exp(tile * scale - line)

    others = pl.ds(0, (count - 1) * block)
    pltpu.make_async_copy(gath.at[others], gath.at[others], gath_recv).wait()

    for c in range(length // lanes):
        column = pl.ds(c * lanes, lanes)
        wide[c] = jnp.exp(gath[:, column].astype(F32))
        for h in range(heads):
            eb[h, column, :] = wide[c, pl.ds(h, length, stride=heads), :].T

    for h in range(heads):
        span = pl.ds(h * length, length)
        total = None
        for i in range(rows):
            weights = e1[i, :, span] * eb[h]
            grad = dp[i, :, span]
            centre = jnp.sum(weights * grad, axis=0, keepdims=True)
            score_grads = weights * (grad - centre)
            p_low[i, :, span] = weights.astype(BF16)
            s_low[i, :, span] = score_grads.astype(BF16)
            total = score_grads if total is None else total + score_grads
        for c in range(length // lanes):
            wide[c, pl.ds(h, length, stride=heads), :] = total[c * lanes:(c + 1) * lanes, :].T
    for c in range(length // lanes):
        terms[:, pl.ds(c * lanes, lanes)] = wide[c].astype(BF16)

    def term_copy(d, t):
        theirs = pl.ds(pl.multiple_of(t * block, block), block)
        return pltpu.make_async_remote_copy(
            src_ref=terms.at[theirs], dst_ref=landed.at[d], send_sem=term_send, recv_sem=term_recv,
            device_id={"row": t},
        )

    peers(me, count, lambda d, t: term_copy(d, t).start())

    for i in range(rows):
        key_part = jnp.dot(s_low[i], qm[i], preferred_element_type=F32)
        kg_ref[i] = (key_part * scale).astype(BF16)
        vg_ref[i] = jnp.dot(p_low[i], gm[i], preferred_element_type=F32).astype(BF16)
        parts = [
            jnp.dot(
                kt[i, pl.ds(h * width, width), :], s_low[i, :, pl.ds(h * length, length)],
                preferred_element_type=F32,
            )
            for h in range(heads)
        ]
        qg_ref[i] = (jnp.concatenate(parts, axis=0).T * scale).astype(BF16)

    arrived = landed.at[pl.ds(1, count - 1)]
    pltpu.make_async_copy(arrived, arrived, term_recv).wait()
    for c in range(length // lanes):
        column = pl.ds(c * lanes, lanes)
        got = jnp.sum(landed[pl.ds(1, count - 1), :, column].astype(F32), axis=0)
        bg_ref[:, column] = wide[c, own, :] + got
    pltpu.make_async_copy(gath.at[others], gath.at[others], gath_send).wait()
    pltpu.make_async_copy(arrived, arrived, term_send).wait()


def local(count, queries, keys, values, grads_out, log_norm, bias):
    rows, length, channels = queries.shape
    bias_rows, heads, _ = bias.shape
    block = bias_rows * heads
    lanes = math.gcd(length, 128)
    any_space = pl.BlockSpec(memory_space=pl.ANY)
    vmem = pl.BlockSpec(memory_space=pltpu.VMEM)
    big = (rows, length, channels)
    outs = pl.pallas_call(
        functools.partial(kernel, count, heads),
        out_shape=(
            jax.ShapeDtypeStruct(big, BF16),
            jax.ShapeDtypeStruct(big, BF16),
            jax.ShapeDtypeStruct(big, BF16),
            jax.ShapeDtypeStruct((block, length), F32),
        ),
        in_specs=[any_space] * 6,
        out_specs=(vmem,) * 4,
        scratch_shapes=[
            pltpu.VMEM(big, BF16),
            pltpu.VMEM(big, BF16),
            pltpu.VMEM(big, BF16),
            pltpu.VMEM(big, BF16),
            pltpu.VMEM((rows * heads, length), F32),
            pltpu.VMEM((count * block, length), BF16),
            pltpu.VMEM((rows, heads * length, channels), BF16),
            pltpu.VMEM((rows, heads * length, channels), BF16),
            pltpu.VMEM((rows, channels, length), BF16),
            pltpu.VMEM((rows, length, heads * length), F32),
            pltpu.VMEM((rows, length, heads * length), F32),
            pltpu.VMEM((heads, length, length), F32),
            pltpu.VMEM((rows, length, heads * length), BF16),
            pltpu.VMEM((rows, length, heads * length), BF16),
            pltpu.VMEM((length // lanes, length * heads, lanes), F32),
            pltpu.VMEM((count * block, length), BF16),
            pltpu.VMEM((count, block, length), BF16),
            pltpu.SemaphoreType.DMA((6,)),
            pltpu.SemaphoreType.DMA,
            pltpu.SemaphoreType.DMA,
            pltpu.SemaphoreType.DMA,
            pltpu.SemaphoreType.DMA,
        ],
        compiler_params=pltpu.CompilerParams(collective_id=0, has_side_effects=True),
    )(
        queries, keys, values, grads_out,
        log_norm.reshape(rows * heads, length), bias.reshape(block, length),
    )
    return outs[0], outs[1], outs[2], outs[3].reshape(bias_rows, heads, length)


def solution(mesh):
    placed = P(("crop", "row"), None, None)
    return jax.shard_map(
        functools.partial(local, mesh.shape["row"]),
        mesh=mesh,
        in_specs=(placed,) * 6,
        out_specs=(placed,) * 4,
        check_vma=False,
    )
```

```python
import functools
import math

import jax
import jax.numpy as jnp
from jax import lax
from jax.experimental import pallas as pl
from jax.experimental.pallas import tpu as pltpu
from jax.sharding import PartitionSpec as P

F32 = jnp.float32
BF16 = jnp.bfloat16


def peers(me, count, body):
    def step(d, carry):
        body(d, lax.rem(me + d, count))
        return carry

    lax.fori_loop(1, count, step, 0)


def kernel(
    count, heads,
    q_hbm, k_hbm, v_hbm, g_hbm, norm_hbm, bias_hbm,
    qg_ref, kg_ref, vg_ref, bg_ref,
    q, k, v, g, norm, gath, qm, gm, kt, e1, dp, eb, p_low, s_low, wide, terms, landed,
    in_sem, gath_send, gath_recv, term_send, term_recv,
):
    me = lax.axis_index("row")
    rows, length, channels = q.shape
    width = channels // heads
    block = bias_hbm.shape[0]
    lanes = wide.shape[2]
    scale = width ** (-0.5)
    own = pl.ds(pl.multiple_of(me * block, block), block)

    barrier = pltpu.get_barrier_semaphore()
    peers(me, count, lambda d, t: pl.semaphore_signal(barrier, inc=1, device_id={"row": t}))

    pairs = ((bias_hbm, gath.at[own]), (q_hbm, q), (k_hbm, k), (v_hbm, v), (g_hbm, g), (norm_hbm, norm))
    copies = [pltpu.make_async_copy(a, b, in_sem.at[i]) for i, (a, b) in enumerate(pairs)]
    for copy in copies:
        copy.start()
    copies[0].wait()
    pl.semaphore_wait(barrier, count - 1)

    def gather_copy(t):
        return pltpu.make_async_remote_copy(
            src_ref=gath.at[own], dst_ref=gath.at[own], send_sem=gath_send, recv_sem=gath_recv,
            device_id={"row": t},
        )

    peers(me, count, lambda d, t: gather_copy(t).start())

    for copy in copies[1:]:
        copy.wait()
    channel = lax.broadcasted_iota(jnp.int32, (1, channels), 1)
    masks = [
        jnp.where((channel >= h * width) & (channel < (h + 1) * width), 1.0, 0.0).astype(BF16)
        for h in range(heads)
    ]
    nt = (((1,), (1,)), ((), ()))
    for i in range(rows):
        for h in range(heads):
            span = pl.ds(h * length, length)
            qm[i, span, :] = q[i] * masks[h]
            gm[i, span, :] = g[i] * masks[h]
        kt[i] = k[i].astype(F32).T.astype(BF16)
        score = lax.dot_general(k[i], qm[i], nt, preferred_element_type=F32)
        grad = lax.dot_general(v[i], gm[i], nt, preferred_element_type=F32)
        dp[i] = grad
        for h in range(heads):
            line = norm[pl.ds(i * heads + h, 1), :]
            tile = score[:, h * length:(h + 1) * length]
            e1[i, :, pl.ds(h * length, length)] = jnp.exp(tile * scale - line)

    others = pl.ds(0, (count - 1) * block)
    pltpu.make_async_copy(gath.at[others], gath.at[others], gath_recv).wait()

    for c in range(length // lanes):
        column = pl.ds(c * lanes, lanes)
        wide[c] = jnp.exp(gath[:, column].astype(F32))
        for h in range(heads):
            eb[h, column, :] = wide[c, pl.ds(h, length, stride=heads), :].T

    for h in range(heads):
        span = pl.ds(h * length, length)
        total = None
        for i in range(rows):
            weights = e1[i, :, span] * eb[h]
            grad = dp[i, :, span]
            centre = jnp.sum(weights * grad, axis=0, keepdims=True)
            score_grads = weights * (grad - centre)
            p_low[i, :, span] = weights.astype(BF16)
            s_low[i, :, span] = score_grads.astype(BF16)
            total = score_grads if total is None else total + score_grads
        for c in range(length // lanes):
            wide[c, pl.ds(h, length, stride=heads), :] = total[c * lanes:(c + 1) * lanes, :].T
    for c in range(length // lanes):
        terms[:, pl.ds(c * lanes, lanes)] = wide[c].astype(BF16)

    def term_copy(d, t):
        theirs = pl.ds(pl.multiple_of(t * block, block), block)
        return pltpu.make_async_remote_copy(
            src_ref=terms.at[theirs], dst_ref=landed.at[d], send_sem=term_send, recv_sem=term_recv,
            device_id={"row": t},
        )

    peers(me, count, lambda d, t: term_copy(d, t).start())

    for i in range(rows):
        key_part = jnp.dot(s_low[i], qm[i], preferred_element_type=F32)
        kg_ref[i] = (key_part * scale).astype(BF16)
        vg_ref[i] = jnp.dot(p_low[i], gm[i], preferred_element_type=F32).astype(BF16)
        parts = [
            jnp.dot(
                kt[i, pl.ds(h * width, width), :], s_low[i, :, pl.ds(h * length, length)],
                preferred_element_type=F32,
            )
            for h in range(heads)
        ]
        qg_ref[i] = (jnp.concatenate(parts, axis=0).T * scale).astype(BF16)

    arrived = landed.at[pl.ds(1, count - 1)]
    pltpu.make_async_copy(arrived, arrived, term_recv).wait()
    for c in range(length // lanes):
        column = pl.ds(c * lanes, lanes)
        got = jnp.sum(landed[pl.ds(1, count - 1), :, column].astype(F32), axis=0)
        bg_ref[:, column] = wide[c, own, :] + got
    pltpu.make_async_copy(gath.at[others], gath.at[others], gath_send).wait()
    pltpu.make_async_copy(arrived, arrived, term_send).wait()


def write_out(*refs):
    half = len(refs) // 2
    sem = refs[-1]
    copies = [pltpu.make_async_copy(refs[i], refs[half + i], sem.at[i]) for i in range(half)]
    for copy in copies:
        copy.start()
    for copy in copies:
        copy.wait()


def local(count, queries, keys, values, grads_out, log_norm, bias):
    rows, length, channels = queries.shape
    bias_rows, heads, _ = bias.shape
    block = bias_rows * heads
    lanes = math.gcd(length, 128)
    any_space = pl.BlockSpec(memory_space=pl.ANY)
    vmem = pl.BlockSpec(memory_space=pltpu.VMEM)
    big = (rows, length, channels)
    shapes = ((big, BF16), (big, BF16), (big, BF16), ((block, length), F32))
    outs = pl.pallas_call(
        functools.partial(kernel, count, heads),
        out_shape=tuple(pltpu.VMEM(*s) for s in shapes),
        in_specs=[any_space] * 6,
        out_specs=(vmem,) * 4,
        scratch_shapes=[
            pltpu.VMEM(big, BF16),
            pltpu.VMEM(big, BF16),
            pltpu.VMEM(big, BF16),
            pltpu.VMEM(big, BF16),
            pltpu.VMEM((rows * heads, length), F32),
            pltpu.VMEM((count * block, length), BF16),
            pltpu.VMEM((rows, heads * length, channels), BF16),
            pltpu.VMEM((rows, heads * length, channels), BF16),
            pltpu.VMEM((rows, channels, length), BF16),
            pltpu.VMEM((rows, length, heads * length), F32),
            pltpu.VMEM((rows, length, heads * length), F32),
            pltpu.VMEM((heads, length, length), F32),
            pltpu.VMEM((rows, length, heads * length), BF16),
            pltpu.VMEM((rows, length, heads * length), BF16),
            pltpu.VMEM((length // lanes, length * heads, lanes), F32),
            pltpu.VMEM((count * block, length), BF16),
            pltpu.VMEM((count, block, length), BF16),
            pltpu.SemaphoreType.DMA((6,)),
            pltpu.SemaphoreType.DMA,
            pltpu.SemaphoreType.DMA,
            pltpu.SemaphoreType.DMA,
            pltpu.SemaphoreType.DMA,
        ],
        compiler_params=pltpu.CompilerParams(collective_id=0, has_side_effects=True),
    )(
        queries, keys, values, grads_out,
        log_norm.reshape(rows * heads, length), bias.reshape(block, length),
    )
    outs = pl.pallas_call(
        write_out,
        out_shape=tuple(jax.ShapeDtypeStruct(*s) for s in shapes),
        in_specs=[vmem] * 4,
        out_specs=(any_space,) * 4,
        scratch_shapes=[pltpu.SemaphoreType.DMA((4,))],
    )(*(pltpu.with_memory_space_constraint(o, pltpu.VMEM) for o in outs))
    return outs[0], outs[1], outs[2], outs[3].reshape(bias_rows, heads, length)


def solution(mesh):
    placed = P(("crop", "row"), None, None)
    return jax.shard_map(
        functools.partial(local, mesh.shape["row"]),
        mesh=mesh,
        in_specs=(placed,) * 6,
        out_specs=(placed,) * 4,
        check_vma=False,
    )
```

```python
import functools
import math

import jax
import jax.numpy as jnp
from jax import lax
from jax.experimental import pallas as pl
from jax.experimental.pallas import tpu as pltpu
from jax.sharding import PartitionSpec as P

F32 = jnp.float32
BF16 = jnp.bfloat16


def ascending(me, count, body):
    def step(at, carry):
        body(at + (at + count - me) // count)
        return carry

    lax.fori_loop(0, count - 1, step, 0)


def descending(me, count, body):
    def step(at, carry):
        back = count - 2 - at
        body(back + (back + count - me) // count)
        return carry

    lax.fori_loop(0, count - 1, step, 0)


def kernel(
    count, heads,
    q_hbm, k_hbm, v_hbm, g_hbm, norm_hbm, bias_hbm,
    qg_ref, kg_ref, vg_ref, bg_ref,
    q, k, v, g, norm, gath, qm, gm, kt, e1, dp, eb, p_low, s_low, wide, terms, landed,
    in_sem, gath_send, gath_recv, term_send, term_recv,
):
    me = lax.axis_index("row")
    rows, length, channels = q.shape
    width = channels // heads
    block = bias_hbm.shape[0]
    lanes = wide.shape[2]
    scale = width ** (-0.5)
    own = pl.ds(pl.multiple_of(me * block, block), block)

    barrier = pltpu.get_barrier_semaphore()
    ascending(me, count, lambda t: pl.semaphore_signal(barrier, inc=1, device_id={"row": t}))

    pairs = ((bias_hbm, gath.at[own]), (q_hbm, q), (k_hbm, k), (v_hbm, v), (g_hbm, g), (norm_hbm, norm))
    copies = [pltpu.make_async_copy(a, b, in_sem.at[i]) for i, (a, b) in enumerate(pairs)]
    for copy in copies:
        copy.start()
    copies[0].wait()
    pl.semaphore_wait(barrier, count - 1)

    def gather_copy(t):
        return pltpu.make_async_remote_copy(
            src_ref=gath.at[own], dst_ref=gath.at[own], send_sem=gath_send, recv_sem=gath_recv,
            device_id={"row": t},
        )

    descending(me, count, lambda t: gather_copy(t).start())

    for copy in copies[1:]:
        copy.wait()
    channel = lax.broadcasted_iota(jnp.int32, (1, channels), 1)
    masks = [
        jnp.where((channel >= h * width) & (channel < (h + 1) * width), 1.0, 0.0).astype(BF16)
        for h in range(heads)
    ]
    nt = (((1,), (1,)), ((), ()))
    for i in range(rows):
        for h in range(heads):
            span = pl.ds(h * length, length)
            qm[i, span, :] = q[i] * masks[h]
            gm[i, span, :] = g[i] * masks[h]
        kt[i] = k[i].astype(F32).T.astype(BF16)
        score = lax.dot_general(k[i], qm[i], nt, preferred_element_type=F32)
        grad = lax.dot_general(v[i], gm[i], nt, preferred_element_type=F32)
        dp[i] = grad
        for h in range(heads):
            line = norm[pl.ds(i * heads + h, 1), :]
            tile = score[:, h * length:(h + 1) * length]
            e1[i, :, pl.ds(h * length, length)] = jnp.exp(tile * scale - line)

    others = pl.ds(0, (count - 1) * block)
    pltpu.make_async_copy(gath.at[others], gath.at[others], gath_recv).wait()

    for c in range(length // lanes):
        column = pl.ds(c * lanes, lanes)
        wide[c] = jnp.exp(gath[:, column].astype(F32))
        for h in range(heads):
            eb[h, column, :] = wide[c, pl.ds(h, length, stride=heads), :].T

    for h in range(heads):
        span = pl.ds(h * length, length)
        total = None
        for i in range(rows):
            weights = e1[i, :, span] * eb[h]
            grad = dp[i, :, span]
            centre = jnp.sum(weights * grad, axis=0, keepdims=True)
            score_grads = weights * (grad - centre)
            p_low[i, :, span] = weights.astype(BF16)
            s_low[i, :, span] = score_grads.astype(BF16)
            total = score_grads if total is None else total + score_grads
        for c in range(length // lanes):
            wide[c, pl.ds(h, length, stride=heads), :] = total[c * lanes:(c + 1) * lanes, :].T
    for c in range(length // lanes):
        terms[:, pl.ds(c * lanes, lanes)] = wide[c].astype(BF16)

    def term_copy(t):
        d = lax.rem(t - me + count, count)
        theirs = pl.ds(pl.multiple_of(t * block, block), block)
        return pltpu.make_async_remote_copy(
            src_ref=terms.at[theirs], dst_ref=landed.at[d], send_sem=term_send, recv_sem=term_recv,
            device_id={"row": t},
        )

    ascending(me, count, lambda t: term_copy(t).start())

    for i in range(rows):
        key_part = jnp.dot(s_low[i], qm[i], preferred_element_type=F32)
        kg_ref[i] = (key_part * scale).astype(BF16)
        vg_ref[i] = jnp.dot(p_low[i], gm[i], preferred_element_type=F32).astype(BF16)
        parts = [
            jnp.dot(
                kt[i, pl.ds(h * width, width), :], s_low[i, :, pl.ds(h * length, length)],
                preferred_element_type=F32,
            )
            for h in range(heads)
        ]
        qg_ref[i] = (jnp.concatenate(parts, axis=0).T * scale).astype(BF16)

    arrived = landed.at[pl.ds(1, count - 1)]
    pltpu.make_async_copy(arrived, arrived, term_recv).wait()
    for c in range(length // lanes):
        column = pl.ds(c * lanes, lanes)
        got = jnp.sum(landed[pl.ds(1, count - 1), :, column].astype(F32), axis=0)
        bg_ref[:, column] = wide[c, own, :] + got
    pltpu.make_async_copy(gath.at[others], gath.at[others], gath_send).wait()
    pltpu.make_async_copy(arrived, arrived, term_send).wait()


def write_out(*refs):
    half = len(refs) // 2
    sem = refs[-1]
    copies = [pltpu.make_async_copy(refs[i], refs[half + i], sem.at[i]) for i in range(half)]
    for copy in copies:
        copy.start()
    for copy in copies:
        copy.wait()


def local(count, queries, keys, values, grads_out, log_norm, bias):
    rows, length, channels = queries.shape
    bias_rows, heads, _ = bias.shape
    block = bias_rows * heads
    lanes = math.gcd(length, 128)
    any_space = pl.BlockSpec(memory_space=pl.ANY)
    vmem = pl.BlockSpec(memory_space=pltpu.VMEM)
    big = (rows, length, channels)
    shapes = ((big, BF16), (big, BF16), (big, BF16), ((block, length), F32))
    outs = pl.pallas_call(
        functools.partial(kernel, count, heads),
        out_shape=tuple(pltpu.VMEM(*s) for s in shapes),
        in_specs=[any_space] * 6,
        out_specs=(vmem,) * 4,
        scratch_shapes=[
            pltpu.VMEM(big, BF16),
            pltpu.VMEM(big, BF16),
            pltpu.VMEM(big, BF16),
            pltpu.VMEM(big, BF16),
            pltpu.VMEM((rows * heads, length), F32),
            pltpu.VMEM((count * block, length), BF16),
            pltpu.VMEM((rows, heads * length, channels), BF16),
            pltpu.VMEM((rows, heads * length, channels), BF16),
            pltpu.VMEM((rows, channels, length), BF16),
            pltpu.VMEM((rows, length, heads * length), F32),
            pltpu.VMEM((rows, length, heads * length), F32),
            pltpu.VMEM((heads, length, length), F32),
            pltpu.VMEM((rows, length, heads * length), BF16),
            pltpu.VMEM((rows, length, heads * length), BF16),
            pltpu.VMEM((length // lanes, length * heads, lanes), F32),
            pltpu.VMEM((count * block, length), BF16),
            pltpu.VMEM((count, block, length), BF16),
            pltpu.SemaphoreType.DMA((6,)),
            pltpu.SemaphoreType.DMA,
            pltpu.SemaphoreType.DMA,
            pltpu.SemaphoreType.DMA,
            pltpu.SemaphoreType.DMA,
        ],
        compiler_params=pltpu.CompilerParams(collective_id=0, has_side_effects=True),
    )(
        queries, keys, values, grads_out,
        log_norm.reshape(rows * heads, length), bias.reshape(block, length),
    )
    outs = pl.pallas_call(
        write_out,
        out_shape=tuple(jax.ShapeDtypeStruct(*s) for s in shapes),
        in_specs=[vmem] * 4,
        out_specs=(any_space,) * 4,
        scratch_shapes=[pltpu.SemaphoreType.DMA((4,))],
    )(*(pltpu.with_memory_space_constraint(o, pltpu.VMEM) for o in outs))
    return outs[0], outs[1], outs[2], outs[3].reshape(bias_rows, heads, length)


def solution(mesh):
    placed = P(("crop", "row"), None, None)
    return jax.shard_map(
        functools.partial(local, mesh.shape["row"]),
        mesh=mesh,
        in_specs=(placed,) * 6,
        out_specs=(placed,) * 4,
        check_vma=False,
    )
```

```python
import functools
import math

import jax
import jax.numpy as jnp
from jax import lax
from jax.experimental import pallas as pl
from jax.experimental.pallas import tpu as pltpu
from jax.sharding import PartitionSpec as P

F32 = jnp.float32
BF16 = jnp.bfloat16


def ascending(me, count, body):
    def step(at, carry):
        body(at + (at + count - me) // count)
        return carry

    lax.fori_loop(0, count - 1, step, 0)


def outside_in(me, count, low_first, body):
    def step(at, carry):
        side = lax.rem(at + low_first, 2)
        near = lax.div(at, 2)
        target = side * near + (1 - side) * (count - 1 - near)

        @pl.when(target != me)
        def _():
            body(target)

        return carry

    lax.fori_loop(0, count, step, 0)


def kernel(
    count, heads,
    q_hbm, k_hbm, v_hbm, g_hbm, norm_hbm, bias_hbm,
    qg_ref, kg_ref, vg_ref, bg_ref,
    q, k, v, g, norm, gath, qm, gm, kt, e1, dp, eb, p_low, s_low, wide, terms, landed,
    in_sem, gath_send, gath_recv, term_send, term_recv,
):
    me = lax.axis_index("row")
    rows, length, channels = q.shape
    width = channels // heads
    block = bias_hbm.shape[0]
    lanes = wide.shape[2]
    scale = width ** (-0.5)
    own = pl.ds(pl.multiple_of(me * block, block), block)

    barrier = pltpu.get_barrier_semaphore()
    ascending(me, count, lambda t: pl.semaphore_signal(barrier, inc=1, device_id={"row": t}))

    pairs = ((bias_hbm, gath.at[own]), (q_hbm, q), (k_hbm, k), (v_hbm, v), (g_hbm, g), (norm_hbm, norm))
    copies = [pltpu.make_async_copy(a, b, in_sem.at[i]) for i, (a, b) in enumerate(pairs)]
    for copy in copies:
        copy.start()
    copies[0].wait()
    pl.semaphore_wait(barrier, count - 1)

    def gather_copy(t):
        return pltpu.make_async_remote_copy(
            src_ref=gath.at[own], dst_ref=gath.at[own], send_sem=gath_send, recv_sem=gath_recv,
            device_id={"row": t},
        )

    outside_in(me, count, 0, lambda t: gather_copy(t).start())

    for copy in copies[1:]:
        copy.wait()
    channel = lax.broadcasted_iota(jnp.int32, (1, channels), 1)
    masks = [
        jnp.where((channel >= h * width) & (channel < (h + 1) * width), 1.0, 0.0).astype(BF16)
        for h in range(heads)
    ]
    nt = (((1,), (1,)), ((), ()))
    for i in range(rows):
        for h in range(heads):
            span = pl.ds(h * length, length)
            qm[i, span, :] = q[i] * masks[h]
            gm[i, span, :] = g[i] * masks[h]
        kt[i] = k[i].astype(F32).T.astype(BF16)
        score = lax.dot_general(k[i], qm[i], nt, preferred_element_type=F32)
        grad = lax.dot_general(v[i], gm[i], nt, preferred_element_type=F32)
        dp[i] = grad
        for h in range(heads):
            line = norm[pl.ds(i * heads + h, 1), :]
            tile = score[:, h * length:(h + 1) * length]
            e1[i, :, pl.ds(h * length, length)] = jnp.exp(tile * scale - line)

    others = pl.ds(0, (count - 1) * block)
    pltpu.make_async_copy(gath.at[others], gath.at[others], gath_recv).wait()

    for c in range(length // lanes):
        column = pl.ds(c * lanes, lanes)
        wide[c] = jnp.exp(gath[:, column].astype(F32))
        for h in range(heads):
            eb[h, column, :] = wide[c, pl.ds(h, length, stride=heads), :].T

    for h in range(heads):
        span = pl.ds(h * length, length)
        total = None
        for i in range(rows):
            weights = e1[i, :, span] * eb[h]
            grad = dp[i, :, span]
            centre = jnp.sum(weights * grad, axis=0, keepdims=True)
            score_grads = weights * (grad - centre)
            p_low[i, :, span] = weights.astype(BF16)
            s_low[i, :, span] = score_grads.astype(BF16)
            total = score_grads if total is None else total + score_grads
        for c in range(length // lanes):
            wide[c, pl.ds(h, length, stride=heads), :] = total[c * lanes:(c + 1) * lanes, :].T
    for c in range(length // lanes):
        terms[:, pl.ds(c * lanes, lanes)] = wide[c].astype(BF16)

    def term_copy(t):
        d = lax.rem(t - me + count, count)
        theirs = pl.ds(pl.multiple_of(t * block, block), block)
        return pltpu.make_async_remote_copy(
            src_ref=terms.at[theirs], dst_ref=landed.at[d], send_sem=term_send, recv_sem=term_recv,
            device_id={"row": t},
        )

    outside_in(me, count, 1, lambda t: term_copy(t).start())

    for i in range(rows):
        key_part = jnp.dot(s_low[i], qm[i], preferred_element_type=F32)
        kg_ref[i] = (key_part * scale).astype(BF16)
        vg_ref[i] = jnp.dot(p_low[i], gm[i], preferred_element_type=F32).astype(BF16)
        parts = [
            jnp.dot(
                kt[i, pl.ds(h * width, width), :], s_low[i, :, pl.ds(h * length, length)],
                preferred_element_type=F32,
            )
            for h in range(heads)
        ]
        qg_ref[i] = (jnp.concatenate(parts, axis=0).T * scale).astype(BF16)

    arrived = landed.at[pl.ds(1, count - 1)]
    pltpu.make_async_copy(arrived, arrived, term_recv).wait()
    for c in range(length // lanes):
        column = pl.ds(c * lanes, lanes)
        got = jnp.sum(landed[pl.ds(1, count - 1), :, column].astype(F32), axis=0)
        bg_ref[:, column] = wide[c, own, :] + got
    pltpu.make_async_copy(gath.at[others], gath.at[others], gath_send).wait()
    pltpu.make_async_copy(arrived, arrived, term_send).wait()


def write_out(*refs):
    half = len(refs) // 2
    sem = refs[-1]
    copies = [pltpu.make_async_copy(refs[i], refs[half + i], sem.at[i]) for i in range(half)]
    for copy in copies:
        copy.start()
    for copy in copies:
        copy.wait()


def local(count, queries, keys, values, grads_out, log_norm, bias):
    rows, length, channels = queries.shape
    bias_rows, heads, _ = bias.shape
    block = bias_rows * heads
    lanes = math.gcd(length, 128)
    any_space = pl.BlockSpec(memory_space=pl.ANY)
    vmem = pl.BlockSpec(memory_space=pltpu.VMEM)
    big = (rows, length, channels)
    shapes = ((big, BF16), (big, BF16), (big, BF16), ((block, length), F32))
    outs = pl.pallas_call(
        functools.partial(kernel, count, heads),
        out_shape=tuple(pltpu.VMEM(*s) for s in shapes),
        in_specs=[any_space] * 6,
        out_specs=(vmem,) * 4,
        scratch_shapes=[
            pltpu.VMEM(big, BF16),
            pltpu.VMEM(big, BF16),
            pltpu.VMEM(big, BF16),
            pltpu.VMEM(big, BF16),
            pltpu.VMEM((rows * heads, length), F32),
            pltpu.VMEM((count * block, length), BF16),
            pltpu.VMEM((rows, heads * length, channels), BF16),
            pltpu.VMEM((rows, heads * length, channels), BF16),
            pltpu.VMEM((rows, channels, length), BF16),
            pltpu.VMEM((rows, length, heads * length), F32),
            pltpu.VMEM((rows, length, heads * length), F32),
            pltpu.VMEM((heads, length, length), F32),
            pltpu.VMEM((rows, length, heads * length), BF16),
            pltpu.VMEM((rows, length, heads * length), BF16),
            pltpu.VMEM((length // lanes, length * heads, lanes), F32),
            pltpu.VMEM((count * block, length), BF16),
            pltpu.VMEM((count, block, length), BF16),
            pltpu.SemaphoreType.DMA((6,)),
            pltpu.SemaphoreType.DMA,
            pltpu.SemaphoreType.DMA,
            pltpu.SemaphoreType.DMA,
            pltpu.SemaphoreType.DMA,
        ],
        compiler_params=pltpu.CompilerParams(collective_id=0, has_side_effects=True),
    )(
        queries, keys, values, grads_out,
        log_norm.reshape(rows * heads, length), bias.reshape(block, length),
    )
    outs = pl.pallas_call(
        write_out,
        out_shape=tuple(jax.ShapeDtypeStruct(*s) for s in shapes),
        in_specs=[vmem] * 4,
        out_specs=(any_space,) * 4,
        scratch_shapes=[pltpu.SemaphoreType.DMA((4,))],
    )(*(pltpu.with_memory_space_constraint(o, pltpu.VMEM) for o in outs))
    return outs[0], outs[1], outs[2], outs[3].reshape(bias_rows, heads, length)


def solution(mesh):
    placed = P(("crop", "row"), None, None)
    return jax.shard_map(
        functools.partial(local, mesh.shape["row"]),
        mesh=mesh,
        in_specs=(placed,) * 6,
        out_specs=(placed,) * 4,
        check_vma=False,
    )
```
